32 devices in a mesh: groups: 1, ep: 32 (over z, y, x, core).
Axes of the slice: x: 2, y: 2, z: 4, core: 2. Of those that a mesh axis runs over, the one named last changes fastest.
Arguments:
- tokens: bfloat16 [2048, 2880], P(('groups', 'ep')), may hold values from -6 to 6
- routes: int32 [2048, 4], P(('groups', 'ep')), may hold values from 0 to 7, all different within a row; in each aligned block of 64 rows (0 to 63, 64 to 127, ...) at most 36 rows name the same one
- norm_gain: bfloat16 [2880], replicated, may hold values from 0.25 to 1.75
- router_weight: bfloat16 [2880, 8], replicated, may hold values from -0.02734375 to 0.02734375
- gate_up_weight: bfloat16 [32, 2880, 720], P('ep'), may hold values from -0.109375 to 0.109375
- down_weight: bfloat16 [32, 360, 2880], P('ep'), may hold values from -0.15625 to 0.15625
Outputs:
- mixed: bfloat16 [2048, 2880], P(('groups', 'ep'))
The draws below stay inside these ranges and needn't reach their ends.
Inputs may be any that keep to these rules, and one draw needn't show every extreme that they name: `routes`: in each aligned block of 64 rows (the rows of one device), no expert is named by more than 36 rows; in some blocks one expert is named by exactly 36 rows. A row names 4 different experts.
All inputs are finite; a program needn't handle non-finite values.
Results may differ from the reference program's by a relative error of at most 0.005.
Values may be sent and summed in bfloat16 or wider, within the bound.
No kernel may reach another device: no remote copies, remote signals or barrier semaphores. Data moves between devices by JAX's collectives and lax.ppermute only.
A program may use at most 128 MiB of HBM per device.

```python
import math
import jax
import jax.numpy as jnp
import numpy as np
from jax import lax

D = 2880
FF_WIN = 1440
TOP = 4
SHARD = 4
TOK_DEV = 64
EXPERTS = 8
FF_DEV = 360
CAP = 36
TOKENS = 2048
N_EP = 32


def level_of(own_key, extent, pieces, least, high):
    def one(axis_at, shards_of):
        steps = jax.random.uniform(jax.random.fold_in(jax.random.fold_in(own_key, 6), axis_at), (shards_of,), jnp.float32, least / len(pieces), high / len(pieces))
        return jnp.repeat(jnp.exp(steps), extent[axis_at] // shards_of).reshape((-1,) + (1,) * (len(extent) - axis_at - 1))

    level = one(*pieces[0])
    for cut in pieces[1:]:
        level = level * one(*cut)
    return level


def assign_block(own_key, own, number, rows, number_of, top, reach, slope):
    order = jax.random.permutation(own_key, number_of)
    heavy_load, usual = load_shares(number_of, rows * top, reach, slope, True), load_shares(number_of, rows * top, reach, slope, False)
    places = jnp.arange(number_of)

    def named(lengths, turn):
        used = int((lengths > 0).sum())
        fixed = max(1, used // 4)
        shifted = fixed + (places - fixed + turn * (used - fixed)) % max(1, number_of - fixed)
        return jnp.zeros((number_of,), jnp.int32).at[order[jnp.where(places < fixed, places, shifted)]].set(jnp.asarray(lengths, jnp.int32))

    lengths = jnp.where(number % 4 == 0, named(heavy_load, number // 4), named(usual, number - number // 4 - 1))
    mixed = jax.random.permutation(jax.random.fold_in(own, 3), number_of)
    source_of, receiver = mixed[0:number_of // 2 * 2:2], mixed[1:number_of // 2 * 2:2]
    margin = jnp.minimum(lengths[source_of] - 1, reach - lengths[receiver]) // 2
    margin = jnp.where((source_of == order[0]) | (receiver == order[0]) | (lengths[receiver] == 0), 0, jnp.maximum(margin, 0))
    shifted = jax.random.randint(jax.random.fold_in(own, 4), (number_of // 2,), 0, 1 << 20) % (margin + 1)
    lengths = lengths.at[source_of].add(-shifted).at[receiver].add(shifted)
    members = jnp.searchsorted(jnp.cumsum(lengths), jnp.arange(rows * top), side="right").astype(jnp.int32)
    table = members.reshape(top, rows).T
    table = table[jax.random.permutation(jax.random.fold_in(own, 1), rows)]
    turn = jax.random.randint(jax.random.fold_in(own, 2), (rows, 1), 0, top)
    return jnp.take_along_axis(table, (jnp.arange(top)[None, :] + turn) % top, axis=1)


def load_shares(number_of, total, reach, lean, full):
    portions = [(1 << 20) // math.isqrt(standing ** lean) + 1 for standing in range(1, number_of + 1)]
    largest = reach if full else min(reach, max(-(-total // number_of), total * portions[0] // sum(portions)))
    least = 1 if total - largest >= number_of - 1 else 0
    given, rest = [largest] + [least] * (number_of - 1), total - largest - least * (number_of - 1)
    while rest > 0:
        free = [i for i in range(1, number_of) if given[i] < largest] or [i for i in range(1, number_of) if given[i] < reach]
        whole, left = sum([portions[i] for i in free]), rest
        for i in free:
            more = min(reach - given[i], max(1, left * portions[i] // whole), rest)
            given[i] = given[i] + more
            rest = rest - more
    return np.array(given)


def centred(stream_key, shape, width, reach, cuts=(), held_as=jnp.bfloat16):
    values = width * jax.random.normal(stream_key, shape, jnp.float32)
    if cuts:
        values = values * level_of(stream_key, shape, cuts, -0.22, 0.18)
    return jnp.clip(values, -reach, reach).astype(held_as)


def setup_inputs(seed: int = 0, part: int = 0) -> dict:
    streams_of = jax.random.split(jax.random.key(seed), 7)
    own_keys = jax.random.split(jax.random.fold_in(streams_of[6], part), 7)
    tokens = centred(own_keys[0], (TOKENS, D), 1.0, 6.0, ((0, 32),))
    routes_keys = jax.random.split(jax.random.fold_in(own_keys[1], 1), TOKENS // TOK_DEV)
    routes_turns = jax.random.permutation(jax.random.fold_in(own_keys[1], 3), TOKENS // TOK_DEV)
    routes = jax.vmap(lambda own, number: assign_block(jax.random.fold_in(own_keys[1], 2), own, number, TOK_DEV, EXPERTS, TOP, CAP, 2))(routes_keys, routes_turns).reshape((TOKENS, TOP))
    norm_gain = jnp.clip(1.0 + 0.15 * jax.random.normal(streams_of[2], (D,), jnp.float32), 0.25, 1.75).astype(jnp.bfloat16)
    router_weight = centred(streams_of[3], (D, EXPERTS), (16 * D) ** -0.5, 0.02734375)
    gate_up_weight = centred(streams_of[4], (EXPERTS * SHARD, D, 2 * FF_DEV), D ** -0.5, 0.109375, ((0, 32),))
    down_weight = centred(streams_of[5], (EXPERTS * SHARD, FF_DEV, D), FF_WIN ** -0.5, 0.15625, ((0, 32),))
    return dict(tokens=tokens, routes=routes, norm_gain=norm_gain, router_weight=router_weight, gate_up_weight=gate_up_weight, down_weight=down_weight)


def reference(tokens, routes, norm_gain, router_weight, gate_up_weight, down_weight):
    stream = tokens.astype(jnp.float32)
    mean_square = lax.optimization_barrier(jnp.mean(stream * stream, axis=-1, keepdims=True))
    normed = (stream * lax.rsqrt(mean_square + 1e-05) * norm_gain.astype(jnp.float32)).astype(jnp.bfloat16)
    logits = jnp.dot(normed, router_weight, preferred_element_type=jnp.float32)
    expert_ids = jnp.arange(EXPERTS, dtype=jnp.int32)
    onehot = routes[:, :, None] == expert_ids[None, None, :]
    chosen = lax.optimization_barrier(jnp.sum(jnp.where(onehot, logits[:, None, :], jnp.float32(0.0)), axis=-1))
    expo = jnp.exp(chosen)
    route_prob = expo / lax.optimization_barrier(jnp.sum(expo, axis=-1, keepdims=True))
    flat_hits = onehot.astype(jnp.int32).reshape(N_EP, TOK_DEV * TOP, EXPERTS)
    rank_before = jnp.cumsum(flat_hits, axis=1) - flat_hits
    slot_index = lax.optimization_barrier(jnp.sum(flat_hits * rank_before, axis=-1)).reshape(TOKENS, TOP).astype(jnp.int32)
    block_ids = (jnp.arange(TOKENS, dtype=jnp.int32) // TOK_DEV)[:, None]
    position = (block_ids * CAP + slot_index).astype(jnp.int32)
    values = jnp.broadcast_to(normed[:, None, :], (TOKENS, TOP, D))
    buffer = jnp.zeros((EXPERTS, N_EP * CAP, D), jnp.bfloat16).at[routes, position].set(values)
    gate_up_all = gate_up_weight.reshape(EXPERTS, SHARD, D, 2 * FF_DEV)
    down_all = down_weight.reshape(EXPERTS, SHARD, FF_DEV, D)

    def one_expert(operands):
        rows, gate_up_part, down_part = operands
        total = jnp.zeros((N_EP * CAP, D), jnp.float32)
        for member in range(SHARD):
            hidden = jnp.dot(rows, gate_up_part[member], preferred_element_type=jnp.float32)
            gate_part = hidden[:, :FF_DEV]
            up_part = hidden[:, FF_DEV:]
            activated = ((up_part + 1.0) * gate_part * jax.nn.sigmoid(1.702 * gate_part)).astype(jnp.bfloat16)
            partial_value = jnp.dot(activated, down_part[member], preferred_element_type=jnp.float32).astype(jnp.bfloat16)
            total = total + partial_value.astype(jnp.float32)
        return total
    expert_sum = lax.map(one_expert, (buffer, gate_up_all, down_all))
    mixture = jnp.zeros((TOKENS, D), jnp.float32)
    for choice_k in range(TOP):
        picked = expert_sum[routes[:, choice_k], position[:, choice_k]]
        mixture = mixture + route_prob[:, choice_k:choice_k + 1] * picked
    return (stream + mixture).astype(jnp.bfloat16)
```

```python
import functools

import jax
import jax.numpy as jnp
from jax import lax
from jax.experimental import pallas as pl
from jax.experimental.pallas import tpu as pltpu
from jax.sharding import PartitionSpec as P

CORES = 2
VMEM_BYTES = 48 * 1024 * 1024


def dot32(a, b, dims=((1,), (0,))):
    return lax.dot_general(a, b, (dims, ((), ())), preferred_element_type=jnp.float32)


def hits_of(routes, experts):
    ids = lax.broadcasted_iota(jnp.int32, (routes.shape[0], experts), 1)
    hits = (routes[:, 0:1] == ids).astype(jnp.float32)
    for k in range(1, routes.shape[1]):
        hits = hits + (routes[:, k : k + 1] == ids).astype(jnp.float32)
    return hits


def normed_of(tokens, gain):
    stream = tokens.astype(jnp.float32)
    mean_square = jnp.mean(stream * stream, axis=-1, keepdims=True)
    return (stream * lax.rsqrt(mean_square + 1e-05) * gain).astype(jnp.bfloat16)


def select_kernel(ids, own, other, routes_own, routes_other, gain, normed, *blocks, experts, cap):
    rows = own.shape[0]
    scale = gain[...].astype(jnp.float32)
    own_core = ids[len(blocks)]
    normed[0:rows, :] = normed_of(own[...], scale)
    normed[rows:, :] = normed_of(other[...], scale)
    before = (
        lax.broadcasted_iota(jnp.int32, (rows, rows), 0)
        < lax.broadcasted_iota(jnp.int32, (rows, rows), 1)
    ).astype(jnp.bfloat16)
    same = (
        lax.broadcasted_iota(jnp.int32, (rows, rows), 0)
        == lax.broadcasted_iota(jnp.int32, (rows, rows), 1)
    ).astype(jnp.bfloat16)
    parts = []
    for which, routes in enumerate((routes_own, routes_other)):
        hits = hits_of(routes[...], experts).astype(jnp.bfloat16)
        slot = dot32(hits, before, ((0,), (0,))).astype(jnp.int32)
        hit = dot32(hits, same, ((0,), (0,)))
        core = own_core if which == 0 else 1 - own_core
        parts.append((slot + core * cap, hit))
    place = jnp.concatenate([p[0] for p in parts], axis=1)
    hit = jnp.concatenate([p[1] for p in parts], axis=1)
    expert_row = lax.broadcasted_iota(jnp.int32, place.shape, 0)
    values = normed[...]
    slots = lax.broadcasted_iota(jnp.int32, (CORES * cap, CORES * rows), 0)
    for m, block in enumerate(blocks):
        mine = expert_row == ids[m]
        at = jnp.sum(jnp.where(mine & (hit > 0.5), place + 1, 0), axis=0, keepdims=True) - 1
        pick = (slots == at).astype(jnp.bfloat16)
        block[...] = dot32(pick, values).astype(jnp.bfloat16)


def weight_kernel(ids, normed, router, routes_own, routes_other, high, low, *, experts, cap):
    rows = routes_own.shape[0]
    count = high.shape[1] // (CORES * cap)
    own_core = ids[count]
    logits = dot32(normed[...], router[...])
    before = (
        lax.broadcasted_iota(jnp.int32, (rows, rows), 1)
        < lax.broadcasted_iota(jnp.int32, (rows, rows), 0)
    ).astype(jnp.bfloat16)
    for which, routes in enumerate((routes_own, routes_other)):
        hits = hits_of(routes[...], experts)
        slot = dot32(before, hits.astype(jnp.bfloat16)).astype(jnp.int32)
        core = own_core if which == 0 else 1 - own_core
        part = logits[which * rows : (which + 1) * rows, :]
        expo = jnp.where(hits > 0.5, jnp.exp(part), 0.0)
        prob = expo / jnp.sum(expo, axis=1, keepdims=True)
        column = lax.broadcasted_iota(jnp.int32, (rows, experts), 1)
        at_lane = lax.broadcasted_iota(jnp.int32, (rows, high.shape[1]), 1)
        total = jnp.zeros((rows, high.shape[1]), jnp.float32)
        for m in range(count):
            mine = column == ids[m]
            weight = jnp.sum(jnp.where(mine, prob, 0.0), axis=1, keepdims=True)
            at = jnp.sum(jnp.where(mine, slot, 0), axis=1, keepdims=True)
            at = at + core * cap + m * CORES * cap
            total = total + jnp.where(at_lane == at, weight, 0.0)
        first = total.astype(jnp.bfloat16)
        high[which * rows : (which + 1) * rows, :] = first
        low[which * rows : (which + 1) * rows, :] = (total - first.astype(jnp.float32)).astype(
            jnp.bfloat16
        )


def expert_kernel(a, b, c, d, gate_up, down, mine_a, mine_b, send, *, ff):
    rows = a.shape[0]
    values = jnp.concatenate([a[...], b[...], c[...], d[...]], axis=0)
    hidden = dot32(values, gate_up[...])
    gate = hidden[:, :ff]
    up = hidden[:, ff:]
    activated = ((up + 1.0) * gate * jax.nn.sigmoid(1.702 * gate)).astype(jnp.bfloat16)
    partial_value = dot32(activated, down[...]).astype(jnp.bfloat16)
    mine_a[...] = partial_value[0:rows]
    mine_b[...] = partial_value[rows : 2 * rows]
    send[...] = partial_value[2 * rows :]


def combine_kernel(high, low, *refs):
    mixed_own, mixed_other = refs[-2], refs[-1]
    values = jnp.concatenate([r[...] for r in refs[:-2]], axis=0)
    mixture = dot32(high[...], values) + dot32(low[...], values)
    rows = mixed_own.shape[0]
    mixed_own[...] = mixture[:rows]
    mixed_other[...] = mixture[rows:].astype(jnp.bfloat16)


def vmem_call(kernel, out_shape, name, scalars=0, count=0):
    specs = [pl.BlockSpec(memory_space=pltpu.SMEM)] * scalars
    specs = specs + [pl.BlockSpec(memory_space=pltpu.VMEM)] * (count - scalars)
    return pl.pallas_call(
        kernel,
        out_shape=out_shape,
        in_specs=specs,
        out_specs=jax.tree.map(lambda _: pl.BlockSpec(memory_space=pltpu.VMEM), out_shape),
        compiler_params=pltpu.CompilerParams(vmem_limit_bytes=VMEM_BYTES),
        name=name,
    )


def shards(tokens, routes, norm_gain, router_weight, gate_up_weight, down_weight):
    rows, width = tokens.shape
    top = routes.shape[1]
    experts = router_weight.shape[1]
    devices = lax.axis_size("ep")
    shard_count = devices // experts
    if shard_count != 2 * CORES or experts % CORES:
        raise ValueError("unsupported mesh")
    ff = down_weight.shape[1]
    cap = min(rows, shard_count * (17 * rows * top // (16 * experts * shard_count) + 1))
    chunks = experts // CORES
    pair = CORES * cap

    index = lax.axis_index("ep")
    core = index % CORES
    expert_high = index // (CORES * shard_count)
    ids = jnp.stack(
        [(expert_high ^ m) * CORES + core for m in range(chunks)] + [core]
    ).astype(jnp.int32)

    def split(i):
        e, s = divmod(i, shard_count)
        return e // CORES, e % CORES, s // CORES, s % CORES

    def join(high, e_low, x, c):
        return ((high * CORES + e_low) * 2 + x) * CORES + c

    far = []
    for m in range(chunks):
        pairs = []
        for i in range(devices):
            high, e_low, x, c = split(i)
            pairs.append((i, join(high ^ m, c, x, e_low)))
        far.append(pairs)
    to_core = [(i, i ^ 1) for i in range(devices)]
    to_x = [(i, i ^ CORES) for i in range(devices)]
    move = functools.partial(lax.ppermute, axis_name="ep")

    other = move(tokens, perm=to_core)
    routes_other = move(routes, perm=to_core)
    block = jax.ShapeDtypeStruct((pair, width), jnp.bfloat16)
    gain = norm_gain.reshape(1, width)
    normed, *blocks = vmem_call(
        functools.partial(select_kernel, experts=experts, cap=cap),
        [jax.ShapeDtypeStruct((CORES * rows, width), jnp.bfloat16)] + [block] * chunks,
        "select",
        1,
        6,
    )(ids, tokens, other, routes, routes_other, gain)

    near = [move(blocks[m], perm=far[m]) for m in range(chunks)]
    weights = jax.ShapeDtypeStruct((CORES * rows, chunks * pair), jnp.bfloat16)
    high, low = vmem_call(
        functools.partial(weight_kernel, experts=experts, cap=cap),
        [weights, weights],
        "weights",
        1,
        5,
    )(ids, normed, router_weight, routes, routes_other)

    gate_up = gate_up_weight[0]
    down = down_weight[0]
    back = []
    for m in range(chunks):
        side = move(near[m], perm=to_x)
        near_other = move(near[m], perm=to_core)
        side_other = move(side, perm=to_core)
        mine, mine_side, send = vmem_call(
            functools.partial(expert_kernel, ff=ff),
            [block, block, jax.ShapeDtypeStruct((2 * pair, width), jnp.bfloat16)],
            f"expert{m}",
            0,
            6,
        )(near[m], side, near_other, side_other, gate_up, down)
        got = move(send, perm=to_core)
        got_mine, got_side = got[:pair], got[pair:]
        out_side = (mine_side.astype(jnp.float32) + got_side.astype(jnp.float32)).astype(
            jnp.bfloat16
        )
        in_side = move(out_side, perm=to_x)
        total = (
            mine.astype(jnp.float32) + got_mine.astype(jnp.float32) + in_side.astype(jnp.float32)
        ).astype(jnp.bfloat16)
        back.append(move(total, perm=far[m]))

    mixed_own, mixed_other = vmem_call(
        combine_kernel,
        [
            jax.ShapeDtypeStruct((rows, width), jnp.float32),
            jax.ShapeDtypeStruct((rows, width), jnp.bfloat16),
        ],
        "combine",
        0,
        2 + chunks,
    )(high, low, *back)
    from_other = move(mixed_other, perm=to_core)
    return (tokens.astype(jnp.float32) + mixed_own + from_other.astype(jnp.float32)).astype(
        jnp.bfloat16
    )


def solution(mesh):
    in_specs = (
        P(("groups", "ep"), None),
        P(("groups", "ep"), None),
        P(),
        P(),
        P("ep", None, None),
        P("ep", None, None),
    )
    out_specs = P(("groups", "ep"), None)
    return jax.shard_map(shards, mesh=mesh, in_specs=in_specs, out_specs=out_specs, check_vma=False)
```

```python
import functools

import jax
import jax.numpy as jnp
from jax import lax
from jax.experimental import pallas as pl
from jax.experimental.pallas import tpu as pltpu
from jax.sharding import PartitionSpec as P


CORES = 2
SHARDS = 4
VMEM_BYTES = 48 * 1024 * 1024


def dot32(a, b, dims=((1,), (0,))):
    return lax.dot_general(a, b, (dims, ((), ())), preferred_element_type=jnp.float32)


def places_of(routes_own, routes_other, own_core, experts, cap):
    places, named = [], []
    for routes, core in ((routes_own, own_core), (routes_other, 1 - own_core)):
        rows = routes.shape[1]
        ids = lax.broadcasted_iota(jnp.int32, (experts, rows), 0)
        hits = (routes[0:1, :] == ids).astype(jnp.float32)
        for k in range(1, routes.shape[0]):
            hits = hits + (routes[k : k + 1, :] == ids).astype(jnp.float32)
        before = (
            lax.broadcasted_iota(jnp.int32, (rows, rows), 0)
            < lax.broadcasted_iota(jnp.int32, (rows, rows), 1)
        ).astype(jnp.bfloat16)
        slot = dot32(hits.astype(jnp.bfloat16), before).astype(jnp.int32)
        places.append(slot + core * cap)
        named.append(hits)
    return jnp.concatenate(places, axis=1), jnp.concatenate(named, axis=1) > 0.5


def at_rows(value, expert):
    mine = lax.broadcasted_iota(jnp.int32, value.shape, 0) == expert
    return jnp.sum(jnp.where(mine, value, jnp.zeros_like(value)), axis=0, keepdims=True)


def normed_of(tokens, gain):
    stream = tokens.astype(jnp.float32)
    mean_square = jnp.mean(stream * stream, axis=-1, keepdims=True)
    return (stream * lax.rsqrt(mean_square + 1e-05) * gain).astype(jnp.bfloat16)


def select_kernel(ids, own, other, routes_own, routes_other, gain, normed, *blocks, experts, cap):
    rows = own.shape[0]
    scale = gain[...].astype(jnp.float32)
    own_core = ids[len(blocks)]
    normed[0:rows, :] = normed_of(own[...], scale)
    normed[rows:, :] = normed_of(other[...], scale)
    place, named = places_of(routes_own[...], routes_other[...], own_core, experts, cap)
    place = jnp.where(named, place + 1, 0)
    values = normed[...]
    slots = lax.broadcasted_iota(jnp.int32, (CORES * cap, CORES * rows), 0) + 1
    for m, block in enumerate(blocks):
        pick = (slots == at_rows(place, ids[m])).astype(jnp.bfloat16)
        block[...] = dot32(pick, values).astype(jnp.bfloat16)


def weight_kernel(ids, normed, router, routes_own, routes_other, high, low, *, experts, cap):
    pair = CORES * cap
    count = high.shape[0] // pair
    logits = dot32(router[...], normed[...], ((1,), (1,)))
    place, named = places_of(routes_own[...], routes_other[...], ids[count], experts, cap)
    expo = jnp.where(named, jnp.exp(logits), 0.0)
    prob = expo / jnp.sum(expo, axis=0, keepdims=True)
    place = jnp.where(named, place + 1, 0)
    slots = lax.broadcasted_iota(jnp.int32, (pair, high.shape[1]), 0) + 1
    for m in range(count):
        here = slots == at_rows(place, ids[m])
        weight = jnp.where(here, at_rows(prob, ids[m]), 0.0)
        first = weight.astype(jnp.bfloat16)
        high[m * pair : (m + 1) * pair, :] = first
        low[m * pair : (m + 1) * pair, :] = (weight - first.astype(jnp.float32)).astype(
            jnp.bfloat16
        )


def expert_kernel(a, b, c, d, gate_up, down, mine_a, mine_b, send, *, ff):
    rows = a.shape[0]
    values = jnp.concatenate([a[...], b[...], c[...], d[...]], axis=0)
    hidden = dot32(values, gate_up[...], ((1,), (1,)))
    gate = hidden[:, :ff]
    up = hidden[:, ff:]
    activated = ((up + 1.0) * gate * jax.nn.sigmoid(1.702 * gate)).astype(jnp.bfloat16)
    partial_value = dot32(activated, down[...]).astype(jnp.bfloat16)
    mine_a[...] = partial_value[0:rows]
    mine_b[...] = partial_value[rows : 2 * rows]
    send[...] = partial_value[2 * rows :]


def combine_kernel(high, low, *refs):
    mixed_own, mixed_other = refs[-2], refs[-1]
    values = jnp.concatenate([r[...] for r in refs[:-2]], axis=0)
    mixture = dot32(high[...], values, ((0,), (0,))) + dot32(low[...], values, ((0,), (0,)))
    rows = mixed_own.shape[0]
    mixed_own[...] = mixture[:rows]
    mixed_other[...] = mixture[rows:].astype(jnp.bfloat16)


def vmem_call(kernel, out_shape, scalars=0, count=0):
    specs = [pl.BlockSpec(memory_space=pltpu.SMEM)] * scalars
    specs = specs + [pl.BlockSpec(memory_space=pltpu.VMEM)] * (count - scalars)
    return pl.pallas_call(
        kernel,
        out_shape=out_shape,
        in_specs=specs,
        out_specs=jax.tree.map(lambda _: pl.BlockSpec(memory_space=pltpu.VMEM), out_shape),
        compiler_params=pltpu.CompilerParams(vmem_limit_bytes=VMEM_BYTES),
    )


def shards(tokens, routes, norm_gain, router_weight, gate_up_weight, down_weight):
    rows, width = tokens.shape
    top = routes.shape[1]
    experts = router_weight.shape[1]
    devices = lax.axis_size("ep")
    shard_count = devices // experts
    if shard_count != SHARDS or experts % CORES:
        raise ValueError("unsupported mesh")
    ff = down_weight.shape[1]
    cap = min(rows, shard_count * (17 * rows * top // (16 * experts * shard_count) + 1))
    chunks = experts // CORES
    pair = CORES * cap

    index = lax.axis_index("ep")
    core = index % CORES
    expert_high = index // (CORES * shard_count)
    ids = jnp.stack(
        [(expert_high ^ m) * CORES + core for m in range(chunks)] + [core]
    ).astype(jnp.int32)

    def split(i):
        e, s = divmod(i, shard_count)
        return e // CORES, e % CORES, s // CORES, s % CORES

    def join(high, e_low, x, c):
        return ((high * CORES + e_low) * 2 + x) * CORES + c

    far = []
    for m in range(chunks):
        pairs = []
        for i in range(devices):
            high, e_low, x, c = split(i)
            pairs.append((i, join(high ^ m, c, x, e_low)))
        far.append(pairs)
    to_core = [(i, i ^ 1) for i in range(devices)]
    to_x = [(i, i ^ CORES) for i in range(devices)]

    def move(value, perm):
        return lax.ppermute(value, "ep", perm)

    other = move(tokens, to_core)
    routes = routes.T
    routes_other = move(routes, to_core)
    block = jax.ShapeDtypeStruct((pair, width), jnp.bfloat16)
    gain = norm_gain.reshape(1, width)
    normed, *blocks = vmem_call(
        functools.partial(select_kernel, experts=experts, cap=cap),
        [jax.ShapeDtypeStruct((CORES * rows, width), jnp.bfloat16)] + [block] * chunks,
        1,
        6,
    )(ids, tokens, other, routes, routes_other, gain)

    near = [move(blocks[m], far[m]) for m in range(chunks)]
    weights = jax.ShapeDtypeStruct((chunks * pair, CORES * rows), jnp.bfloat16)
    high, low = vmem_call(
        functools.partial(weight_kernel, experts=experts, cap=cap), [weights, weights], 1, 5
    )(ids, normed, router_weight.T, routes, routes_other)

    gate_up = gate_up_weight[0].T
    down = down_weight[0]
    back = []
    for m in range(chunks):
        side = move(near[m], to_x)
        near_other = move(near[m], to_core)
        side_other = move(side, to_core)
        mine, mine_side, send = vmem_call(
            functools.partial(expert_kernel, ff=ff),
            [block, block, jax.ShapeDtypeStruct((2 * pair, width), jnp.bfloat16)],
            0,
            6,
        )(near[m], side, near_other, side_other, gate_up, down)
        got = move(send, to_core)
        got_mine, got_side = got[:pair], got[pair:]
        out_side = (mine_side.astype(jnp.float32) + got_side.astype(jnp.float32)).astype(
            jnp.bfloat16
        )
        in_side = move(out_side, to_x)
        total = (
            mine.astype(jnp.float32) + got_mine.astype(jnp.float32) + in_side.astype(jnp.float32)
        ).astype(jnp.bfloat16)
        back.append(move(total, far[m]))

    mixed_own, mixed_other = vmem_call(
        combine_kernel,
        [
            jax.ShapeDtypeStruct((rows, width), jnp.float32),
            jax.ShapeDtypeStruct((rows, width), jnp.bfloat16),
        ],
        0,
        2 + chunks,
    )(high, low, *back)
    from_other = move(mixed_other, to_core)
    return (tokens.astype(jnp.float32) + mixed_own + from_other.astype(jnp.float32)).astype(
        jnp.bfloat16
    )


def solution(mesh):
    in_specs = (
        P(("groups", "ep"), None),
        P(("groups", "ep"), None),
        P(),
        P(),
        P("ep", None, None),
        P("ep", None, None),
    )
    out_specs = P(("groups", "ep"), None)
    return jax.shard_map(shards, mesh=mesh, in_specs=in_specs, out_specs=out_specs, check_vma=False)
```

```python
import functools

import jax
import jax.numpy as jnp
from jax import lax
from jax.experimental import pallas as pl
from jax.experimental.pallas import tpu as pltpu
from jax.sharding import PartitionSpec as P


CORES = 2
SHARDS = 4
NEAR = 2
VMEM_BYTES = 48 * 1024 * 1024


def dot32(a, b, dims=((1,), (0,))):
    return lax.dot_general(a, b, (dims, ((), ())), preferred_element_type=jnp.float32)


def places_of(routes_by_core, own_core, experts, cap):
    places = []
    for routes, core in zip(routes_by_core, (own_core, 1 - own_core)):
        rows = routes.shape[1]
        ids = lax.broadcasted_iota(jnp.int32, (experts, rows), 0)
        hits = (routes[0:1, :] == ids).astype(jnp.float32)
        for k in range(1, routes.shape[0]):
            hits = hits + (routes[k : k + 1, :] == ids).astype(jnp.float32)
        before = (
            lax.broadcasted_iota(jnp.int32, (rows, rows), 0)
            < lax.broadcasted_iota(jnp.int32, (rows, rows), 1)
        ).astype(jnp.bfloat16)
        slot = dot32(hits.astype(jnp.bfloat16), before).astype(jnp.int32)
        places.append(jnp.where(hits > 0.5, slot + core * cap + 1, 0))
    return jnp.concatenate(places, axis=1)


def at_rows(value, expert):
    mine = lax.broadcasted_iota(jnp.int32, value.shape, 0) == expert
    return jnp.sum(jnp.where(mine, value, jnp.zeros_like(value)), axis=0, keepdims=True)


def normed_of(tokens, gain):
    stream = tokens.astype(jnp.float32)
    mean_square = jnp.mean(stream * stream, axis=-1, keepdims=True)
    return (stream * lax.rsqrt(mean_square + 1e-05) * gain).astype(jnp.bfloat16)


def block_rows(rows, tokens):
    return lax.broadcasted_iota(jnp.int32, (rows, tokens), 0) + 1


def select_far(ids, own, other, routes_own, routes_other, gain, normed, *blocks, experts, cap):
    rows = own.shape[0]
    scale = gain[...].astype(jnp.float32)
    normed[0:rows, :] = normed_of(own[...], scale)
    normed[rows:, :] = normed_of(other[...], scale)
    place = places_of((routes_own[...], routes_other[...]), ids[NEAR + len(blocks)], experts, cap)
    values = normed[...]
    slots = block_rows(CORES * cap, CORES * rows)
    for m, block in enumerate(blocks):
        pick = (slots == at_rows(place, ids[NEAR + m])).astype(jnp.bfloat16)
        block[...] = dot32(pick, values).astype(jnp.bfloat16)


def both_places(ids_core, routes, routes_side, experts, cap):
    top = routes.shape[0] // CORES
    place = places_of((routes[:top, :], routes[top:, :]), ids_core, experts, cap)
    side = places_of((routes_side[:top, :], routes_side[top:, :]), ids_core, experts, cap)
    side = jnp.where(side > 0, side + CORES * cap, 0)
    return place, side


def select_near(ids, normed, side, side_other, routes, routes_side, gain, *refs, experts, cap):
    all_normed, blocks = refs[0], refs[1:]
    rows = side.shape[0]
    scale = gain[...].astype(jnp.float32)
    all_normed[0 : 2 * rows, :] = normed[...]
    all_normed[2 * rows : 3 * rows, :] = normed_of(side[...], scale)
    all_normed[3 * rows :, :] = normed_of(side_other[...], scale)
    core = ids[ids.shape[0] - 1]
    place = jnp.concatenate(both_places(core, routes[...], routes_side[...], experts, cap), axis=1)
    values = all_normed[...]
    slots = block_rows(2 * CORES * cap, 2 * CORES * rows)
    for m, block in enumerate(blocks):
        pick = (slots == at_rows(place, ids[m])).astype(jnp.bfloat16)
        block[...] = dot32(pick, values).astype(jnp.bfloat16)


def store_weight(high, low, at, weight):
    first = weight.astype(jnp.bfloat16)
    high[at, :] = first
    low[at, :] = (weight - first.astype(jnp.float32)).astype(jnp.bfloat16)


def weight_kernel(ids, normed, router, routes, routes_side, *refs, experts, cap):
    near_high, near_low, far_high, far_low = refs
    pair = CORES * cap
    core = ids[ids.shape[0] - 1]
    tokens = far_high.shape[1]
    logits = dot32(router[...], normed[...], ((1,), (1,)))
    own_place, side_place = both_places(core, routes[...], routes_side[...], experts, cap)
    place = jnp.concatenate([own_place, side_place], axis=1)
    expo = jnp.where(place > 0, jnp.exp(logits), 0.0)
    prob = expo / jnp.sum(expo, axis=0, keepdims=True)
    slots = block_rows(2 * pair, 2 * tokens)
    for m in range(NEAR):
        here = slots == at_rows(place, ids[m])
        weight = jnp.where(here, at_rows(prob, ids[m]), 0.0)
        store_weight(near_high, near_low, slice(m * 2 * pair, (m + 1) * 2 * pair), weight)
    slots = block_rows(pair, tokens)
    for m in range(far_high.shape[0] // pair):
        here = slots == at_rows(own_place, ids[NEAR + m])
        weight = jnp.where(here, at_rows(prob[:, :tokens], ids[NEAR + m]), 0.0)
        store_weight(far_high, far_low, slice(m * pair, (m + 1) * pair), weight)


def expert_kernel(*refs, ff, blocks):
    gate_up, down = refs[blocks], refs[blocks + 1]
    mine, send = refs[blocks + 2 : -1], refs[-1]
    values = jnp.concatenate([r[...] for r in refs[:blocks]], axis=0)
    hidden = dot32(values, gate_up[...], ((1,), (1,)))
    gate = hidden[:, :ff]
    up = hidden[:, ff:]
    activated = ((up + 1.0) * gate * jax.nn.sigmoid(1.702 * gate)).astype(jnp.bfloat16)
    partial_value = dot32(activated, down[...]).astype(jnp.bfloat16)
    at = 0
    for r in (*mine, send):
        r[...] = partial_value[at : at + r.shape[0]]
        at = at + r.shape[0]


def weighted(high, low, values):
    values = jnp.concatenate([r[...] for r in values], axis=0)
    dims = ((0,), (0,))
    return dot32(high[...], values, dims) + dot32(low[...], values, dims)


def combine_near(high, low, *refs):
    mixture = weighted(high, low, refs[:NEAR])
    at = 0
    for r in refs[NEAR:]:
        r[...] = mixture[at : at + r.shape[0]].astype(r.dtype)
        at = at + r.shape[0]


def combine_far(high, low, near_own, near_other, *refs):
    mixed_own, mixed_other = refs[-2], refs[-1]
    mixture = weighted(high, low, refs[:-2])
    rows = mixed_own.shape[0]
    mixed_own[...] = mixture[:rows] + near_own[...]
    mixed_other[...] = (mixture[rows:] + near_other[...]).astype(jnp.bfloat16)


def vmem_call(kernel, out_shape, scalars=0, count=0):
    specs = [pl.BlockSpec(memory_space=pltpu.SMEM)] * scalars
    specs = specs + [pl.BlockSpec(memory_space=pltpu.VMEM)] * (count - scalars)
    return pl.pallas_call(
        kernel,
        out_shape=out_shape,
        in_specs=specs,
        out_specs=jax.tree.map(lambda _: pl.BlockSpec(memory_space=pltpu.VMEM), out_shape),
        compiler_params=pltpu.CompilerParams(vmem_limit_bytes=VMEM_BYTES),
    )


def shards(tokens, routes, norm_gain, router_weight, gate_up_weight, down_weight):
    rows, width = tokens.shape
    top = routes.shape[1]
    experts = router_weight.shape[1]
    devices = lax.axis_size("ep")
    shard_count = devices // experts
    if shard_count != SHARDS or experts % CORES:
        raise ValueError("unsupported mesh")
    ff = down_weight.shape[1]
    cap = min(rows, shard_count * (17 * rows * top // (16 * experts * shard_count) + 1))
    chunks = experts // CORES
    pair = CORES * cap

    index = lax.axis_index("ep")
    core = index % CORES
    expert_high = index // (CORES * shard_count)
    ids = jnp.stack(
        [(expert_high ^ m) * CORES + core for m in range(chunks)] + [core]
    ).astype(jnp.int32)

    def split(i):
        e, s = divmod(i, shard_count)
        return e // CORES, e % CORES, s // CORES, s % CORES

    def join(high, e_low, x, c):
        return ((high * CORES + e_low) * 2 + x) * CORES + c

    far = []
    for m in range(chunks):
        pairs = []
        for i in range(devices):
            high, e_low, x, c = split(i)
            pairs.append((i, join(high ^ m, c, x, e_low)))
        far.append(pairs)
    to_core = [(i, i ^ 1) for i in range(devices)]
    to_x = [(i, i ^ CORES) for i in range(devices)]

    def move(value, perm):
        return lax.ppermute(value, "ep", perm)

    other = move(tokens, to_core)
    routes = routes.T
    routes_other = move(routes, to_core)
    side = move(tokens, to_x)
    both_routes = jnp.concatenate([routes, routes_other], axis=0)
    side_routes = move(both_routes, to_x)
    bf16 = functools.partial(jax.ShapeDtypeStruct, dtype=jnp.bfloat16)
    f32 = functools.partial(jax.ShapeDtypeStruct, dtype=jnp.float32)
    block, double = bf16((pair, width)), bf16((2 * pair, width))
    gain = norm_gain.reshape(1, width)
    sizes = dict(experts=experts, cap=cap)
    normed, *blocks = vmem_call(
        functools.partial(select_far, **sizes),
        [bf16((CORES * rows, width))] + [block] * (chunks - NEAR),
        1,
        6,
    )(ids, tokens, other, routes, routes_other, gain)
    sent = [None] * NEAR + [move(blocks[m - NEAR], far[m]) for m in range(NEAR, chunks)]
    all_normed, *blocks = vmem_call(
        functools.partial(select_near, **sizes),
        [bf16((2 * CORES * rows, width))] + [double] * NEAR,
        1,
        7,
    )(ids, normed, side, move(side, to_core), both_routes, side_routes, gain)
    for m in range(NEAR):
        sent[m] = move(blocks[m], far[m])
    near_weights = bf16((NEAR * 2 * pair, 2 * CORES * rows))
    far_weights = bf16(((chunks - NEAR) * pair, CORES * rows))
    near_high, near_low, far_high, far_low = vmem_call(
        functools.partial(weight_kernel, **sizes),
        [near_weights, near_weights, far_weights, far_weights],
        1,
        5,
    )(ids, all_normed, router_weight.T, both_routes, side_routes)

    gate_up = gate_up_weight[0].T
    down = down_weight[0]
    wide = jnp.float32
    back = []
    for m in range(chunks):
        if m < NEAR:
            mine, send = vmem_call(
                functools.partial(expert_kernel, ff=ff, blocks=2), [double, double], 0, 4
            )(sent[m], move(sent[m], to_core), gate_up, down)
            got = move(send, to_core)
            total = (mine.astype(wide) + got.astype(wide)).astype(jnp.bfloat16)
        else:
            across = move(sent[m], to_x)
            sent_other = move(sent[m], to_core)
            across_other = move(across, to_core)
            mine, mine_side, send = vmem_call(
                functools.partial(expert_kernel, ff=ff, blocks=4), [block, block, double], 0, 6
            )(sent[m], across, sent_other, across_other, gate_up, down)
            got = move(send, to_core)
            got_mine, got_side = got[:pair], got[pair:]
            out_side = (mine_side.astype(wide) + got_side.astype(wide)).astype(jnp.bfloat16)
            in_side = move(out_side, to_x)
            total = (mine.astype(wide) + got_mine.astype(wide) + in_side.astype(wide)).astype(
                jnp.bfloat16
            )
        back.append(move(total, far[m]))

    part = f32((rows, width))
    near_own, near_other, near_side, near_side_other = vmem_call(
        combine_near, [part, part, part, bf16((rows, width))], 0, 2 + NEAR
    )(near_high, near_low, *back[:NEAR])
    got = move(near_side_other, to_core)
    from_side = move((near_side + got.astype(wide)).astype(jnp.bfloat16), to_x)
    mixed_own, mixed_other = vmem_call(
        combine_far, [part, bf16((rows, width))], 0, 4 + chunks - NEAR
    )(far_high, far_low, near_own, near_other, *back[NEAR:])
    from_other = move(mixed_other, to_core)
    mixed = mixed_own + from_side.astype(wide) + from_other.astype(wide)
    return (tokens.astype(wide) + mixed).astype(jnp.bfloat16)


def solution(mesh):
    in_specs = (
        P(("groups", "ep"), None),
        P(("groups", "ep"), None),
        P(),
        P(),
        P("ep", None, None),
        P("ep", None, None),
    )
    out_specs = P(("groups", "ep"), None)
    return jax.shard_map(shards, mesh=mesh, in_specs=in_specs, out_specs=out_specs, check_vma=False)
```

```python
import functools

import jax
import jax.numpy as jnp
from jax import lax
from jax.experimental import pallas as pl
from jax.experimental.pallas import tpu as pltpu
from jax.sharding import PartitionSpec as P


CORES = 2
SHARDS = 4
NEAR = 2
VMEM_BYTES = 48 * 1024 * 1024


def dot32(a, b, dims=((1,), (0,))):
    return lax.dot_general(a, b, (dims, ((), ())), preferred_element_type=jnp.float32)


def places_of(routes_own, routes_other, own_core, experts, cap):
    places, named = [], []
    for routes, core in ((routes_own, own_core), (routes_other, 1 - own_core)):
        rows = routes.shape[1]
        ids = lax.broadcasted_iota(jnp.int32, (experts, rows), 0)
        hits = (routes[0:1, :] == ids).astype(jnp.float32)
        for k in range(1, routes.shape[0]):
            hits = hits + (routes[k : k + 1, :] == ids).astype(jnp.float32)
        before = (
            lax.broadcasted_iota(jnp.int32, (rows, rows), 0)
            < lax.broadcasted_iota(jnp.int32, (rows, rows), 1)
        ).astype(jnp.bfloat16)
        slot = dot32(hits.astype(jnp.bfloat16), before).astype(jnp.int32)
        places.append(slot + core * cap)
        named.append(hits)
    return jnp.concatenate(places, axis=1), jnp.concatenate(named, axis=1) > 0.5


def at_rows(value, expert):
    mine = lax.broadcasted_iota(jnp.int32, value.shape, 0) == expert
    return jnp.sum(jnp.where(mine, value, jnp.zeros_like(value)), axis=0, keepdims=True)


def normed_of(tokens, gain):
    stream = tokens.astype(jnp.float32)
    mean_square = jnp.mean(stream * stream, axis=-1, keepdims=True)
    return (stream * lax.rsqrt(mean_square + 1e-05) * gain).astype(jnp.bfloat16)


def select_kernel(ids, own, other, routes, gain, normed, *blocks, experts, cap):
    rows = own.shape[0]
    top = routes.shape[0] // CORES
    scale = gain[...].astype(jnp.float32)
    own_core = ids[ids.shape[0] - 1]
    normed[0:rows, :] = normed_of(own[...], scale)
    normed[rows:, :] = normed_of(other[...], scale)
    place, named = places_of(routes[0:top, :], routes[top:, :], own_core, experts, cap)
    place = jnp.where(named, place + 1, 0)
    values = normed[...]
    slots = lax.broadcasted_iota(jnp.int32, (CORES * cap, CORES * rows), 0) + 1
    for m, block in enumerate(blocks):
        pick = (slots == at_rows(place, ids[m])).astype(jnp.bfloat16)
        block[...] = dot32(pick, values).astype(jnp.bfloat16)


def weight_kernel(ids, normed, router, routes, high, low, *, experts, cap):
    pair = CORES * cap
    count = high.shape[0] // pair
    logits = dot32(router[...], normed[...], ((1,), (1,)))
    top = routes.shape[0] // CORES
    place, named = places_of(routes[0:top, :], routes[top:, :], ids[count], experts, cap)
    expo = jnp.where(named, jnp.exp(logits), 0.0)
    prob = expo / jnp.sum(expo, axis=0, keepdims=True)
    place = jnp.where(named, place + 1, 0)
    slots = lax.broadcasted_iota(jnp.int32, (pair, high.shape[1]), 0) + 1
    for m in range(count):
        here = slots == at_rows(place, ids[m])
        weight = jnp.where(here, at_rows(prob, ids[m]), 0.0)
        first = weight.astype(jnp.bfloat16)
        high[m * pair : (m + 1) * pair, :] = first
        low[m * pair : (m + 1) * pair, :] = (weight - first.astype(jnp.float32)).astype(
            jnp.bfloat16
        )


def expert_kernel(a, b, c, d, gate_up, down, mine_a, mine_b, send, *, ff):
    rows = a.shape[0]
    values = jnp.concatenate([a[...], b[...], c[...], d[...]], axis=0)
    hidden = dot32(values, gate_up[...], ((1,), (1,)))
    gate = hidden[:, :ff]
    up = hidden[:, ff:]
    activated = ((up + 1.0) * gate * jax.nn.sigmoid(1.702 * gate)).astype(jnp.bfloat16)
    partial_value = dot32(activated, down[...]).astype(jnp.bfloat16)
    mine_a[...] = partial_value[0:rows]
    mine_b[...] = partial_value[rows : 2 * rows]
    send[...] = partial_value[2 * rows :]


def combine_kernel(high, low, *refs):
    mixed_own, mixed_other = refs[-2], refs[-1]
    values = jnp.concatenate([r[...] for r in refs[:-2]], axis=0)
    mixture = dot32(high[...], values, ((0,), (0,))) + dot32(low[...], values, ((0,), (0,)))
    rows = mixed_own.shape[0]
    mixed_own[...] = mixture[:rows]
    mixed_other[...] = mixture[rows:].astype(jnp.bfloat16)


def vmem_call(kernel, out_shape, scalars=0, count=0):
    specs = [pl.BlockSpec(memory_space=pltpu.SMEM)] * scalars
    specs = specs + [pl.BlockSpec(memory_space=pltpu.VMEM)] * (count - scalars)
    return pl.pallas_call(
        kernel,
        out_shape=out_shape,
        in_specs=specs,
        out_specs=jax.tree.map(lambda _: pl.BlockSpec(memory_space=pltpu.VMEM), out_shape),
        compiler_params=pltpu.CompilerParams(vmem_limit_bytes=VMEM_BYTES),
    )


def shards(tokens, routes, norm_gain, router_weight, gate_up_weight, down_weight):
    rows, width = tokens.shape
    top = routes.shape[1]
    experts = router_weight.shape[1]
    devices = lax.axis_size("ep")
    shard_count = devices // experts
    if shard_count != SHARDS or experts % CORES:
        raise ValueError("unsupported mesh")
    ff = down_weight.shape[1]
    cap = min(rows, shard_count * (17 * rows * top // (16 * experts * shard_count) + 1))
    chunks = experts // CORES
    pair = CORES * cap

    index = lax.axis_index("ep")
    core = index % CORES
    expert_high = index // (CORES * shard_count)
    ids = jnp.stack(
        [(expert_high ^ m) * CORES + core for m in range(chunks)] + [core]
    ).astype(jnp.int32)

    def split(i):
        e, s = divmod(i, shard_count)
        return e // CORES, e % CORES, s // CORES, s % CORES

    def join(high, e_low, x, c):
        return ((high * CORES + e_low) * 2 + x) * CORES + c

    far = []
    for m in range(chunks):
        pairs = []
        for i in range(devices):
            high, e_low, x, c = split(i)
            pairs.append((i, join(high ^ m, c, x, e_low)))
        far.append(pairs)
    to_core = [(i, i ^ 1) for i in range(devices)]
    to_x = [(i, i ^ CORES) for i in range(devices)]

    def move(value, perm):
        return lax.ppermute(value, "ep", perm)

    other = move(tokens, to_core)
    routes = routes.T
    routes = jnp.concatenate([routes, move(routes, to_core)], axis=0)
    block = jax.ShapeDtypeStruct((pair, width), jnp.bfloat16)
    gain = norm_gain.reshape(1, width)

    def select(own, other, routes):
        return vmem_call(
            functools.partial(select_kernel, experts=experts, cap=cap),
            [jax.ShapeDtypeStruct((CORES * rows, width), jnp.bfloat16)] + [block] * NEAR,
            1,
            5,
        )(ids, own, other, routes, gain)

    lent = {}
    for m in range(NEAR, chunks, NEAR):
        pairs = []
        for i in range(devices):
            high, e_low, x, c = split(i)
            pairs.append((i, join(high ^ m, e_low, x, c)))
        lent[m] = (move(tokens, pairs), move(routes, pairs))
    normed, *blocks = select(tokens, other, routes)
    near = [move(blocks[n], far[n]) for n in range(NEAR)]
    for (theirs, their_routes) in lent.values():
        _, *blocks = select(theirs, move(theirs, to_core), their_routes)
        near += [move(blocks[n], far[n]) for n in range(NEAR)]
    weights = jax.ShapeDtypeStruct((chunks * pair, CORES * rows), jnp.bfloat16)
    high, low = vmem_call(
        functools.partial(weight_kernel, experts=experts, cap=cap), [weights, weights], 1, 4
    )(ids, normed, router_weight.T, routes)

    gate_up = gate_up_weight[0].T
    down = down_weight[0]
    back = []
    for m in range(chunks):
        side = move(near[m], to_x)
        near_other = move(near[m], to_core)
        side_other = move(side, to_core)
        mine, mine_side, send = vmem_call(
            functools.partial(expert_kernel, ff=ff),
            [block, block, jax.ShapeDtypeStruct((2 * pair, width), jnp.bfloat16)],
            0,
            6,
        )(near[m], side, near_other, side_other, gate_up, down)
        got = move(send, to_core)
        got_mine, got_side = got[:pair], got[pair:]
        out_side = (mine_side.astype(jnp.float32) + got_side.astype(jnp.float32)).astype(
            jnp.bfloat16
        )
        in_side = move(out_side, to_x)
        total = (
            mine.astype(jnp.float32) + got_mine.astype(jnp.float32) + in_side.astype(jnp.float32)
        ).astype(jnp.bfloat16)
        back.append(move(total, far[m]))

    mixed_own, mixed_other = vmem_call(
        combine_kernel,
        [
            jax.ShapeDtypeStruct((rows, width), jnp.float32),
            jax.ShapeDtypeStruct((rows, width), jnp.bfloat16),
        ],
        0,
        2 + chunks,
    )(high, low, *back)
    from_other = move(mixed_other, to_core)
    return (tokens.astype(jnp.float32) + mixed_own + from_other.astype(jnp.float32)).astype(
        jnp.bfloat16
    )


def solution(mesh):
    in_specs = (
        P(("groups", "ep"), None),
        P(("groups", "ep"), None),
        P(),
        P(),
        P("ep", None, None),
        P("ep", None, None),
    )
    out_specs = P(("groups", "ep"), None)
    return jax.shard_map(shards, mesh=mesh, in_specs=in_specs, out_specs=out_specs, check_vma=False)
```

```python
import functools

import jax
import jax.numpy as jnp
from jax import lax
from jax.experimental import pallas as pl
from jax.experimental.pallas import tpu as pltpu
from jax.sharding import PartitionSpec as P


CORES = 2
SHARDS = 4
VMEM_BYTES = 16 * 1024 * 1024


def dot32(a, b, dims=((1,), (0,))):
    return lax.dot_general(a, b, (dims, ((), ())), preferred_element_type=jnp.float32)


def places_of(routes_own, routes_other, own_core, experts, cap):
    places, named = [], []
    for routes, core in ((routes_own, own_core), (routes_other, 1 - own_core)):
        rows = routes.shape[1]
        ids = lax.broadcasted_iota(jnp.int32, (experts, rows), 0)
        hits = (routes[0:1, :] == ids).astype(jnp.float32)
        for k in range(1, routes.shape[0]):
            hits = hits + (routes[k : k + 1, :] == ids).astype(jnp.float32)
        before = (
            lax.broadcasted_iota(jnp.int32, (rows, rows), 0)
            < lax.broadcasted_iota(jnp.int32, (rows, rows), 1)
        ).astype(jnp.bfloat16)
        slot = dot32(hits.astype(jnp.bfloat16), before).astype(jnp.int32)
        places.append(slot + core * cap)
        named.append(hits)
    return jnp.concatenate(places, axis=1), jnp.concatenate(named, axis=1) > 0.5


def at_rows(value, expert):
    mine = lax.broadcasted_iota(jnp.int32, value.shape, 0) == expert
    return jnp.sum(jnp.where(mine, value, jnp.zeros_like(value)), axis=0, keepdims=True)


def normed_of(tokens, gain):
    stream = tokens.astype(jnp.float32)
    mean_square = jnp.mean(stream * stream, axis=-1, keepdims=True)
    return (stream * lax.rsqrt(mean_square + 1e-05) * gain).astype(jnp.bfloat16)


def select_kernel(ids, own, other, routes_own, routes_other, gain, normed, *blocks, experts, cap):
    rows = own.shape[0]
    scale = gain[...].astype(jnp.float32)
    own_core = ids[len(blocks)]
    normed[0:rows, :] = normed_of(own[...], scale)
    normed[rows:, :] = normed_of(other[...], scale)
    place, named = places_of(routes_own[...], routes_other[...], own_core, experts, cap)
    place = jnp.where(named, place + 1, 0)
    values = normed[...]
    slots = lax.broadcasted_iota(jnp.int32, (CORES * cap, CORES * rows), 0) + 1
    for m, block in enumerate(blocks):
        pick = (slots == at_rows(place, ids[m])).astype(jnp.bfloat16)
        block[...] = dot32(pick, values).astype(jnp.bfloat16)


def weight_kernel(ids, normed, router, routes_own, routes_other, high, low, *, experts, cap):
    pair = CORES * cap
    count = high.shape[0] // pair
    logits = dot32(router[...], normed[...], ((1,), (1,)))
    place, named = places_of(routes_own[...], routes_other[...], ids[count], experts, cap)
    expo = jnp.where(named, jnp.exp(logits), 0.0)
    prob = expo / jnp.sum(expo, axis=0, keepdims=True)
    place = jnp.where(named, place + 1, 0)
    slots = lax.broadcasted_iota(jnp.int32, (pair, high.shape[1]), 0) + 1
    for m in range(count):
        here = slots == at_rows(place, ids[m])
        weight = jnp.where(here, at_rows(prob, ids[m]), 0.0)
        first = weight.astype(jnp.bfloat16)
        high[m * pair : (m + 1) * pair, :] = first
        low[m * pair : (m + 1) * pair, :] = (weight - first.astype(jnp.float32)).astype(
            jnp.bfloat16
        )


def turn_kernel(stored, turned):
    turned[...] = stored[...].T


def expert_kernel(mine_in, other_in, gate_up, down, mine, send, *, ff):
    rows = mine.shape[0]
    values = jnp.concatenate([mine_in[...], other_in[...]], axis=0)
    hidden = dot32(values, gate_up[...])
    gate = hidden[:, :ff]
    up = hidden[:, ff:]
    activated = ((up + 1.0) * gate * jax.nn.sigmoid(1.702 * gate)).astype(jnp.bfloat16)
    partial_value = dot32(activated, down[...]).astype(jnp.bfloat16)
    mine[...] = partial_value[:rows]
    send[...] = partial_value[rows:]


def combine_kernel(high, low, *refs):
    mixed_own, mixed_other = refs[-2], refs[-1]
    values = jnp.concatenate([r[...] for r in refs[:-2]], axis=0)
    mixture = dot32(high[...], values, ((0,), (0,))) + dot32(low[...], values, ((0,), (0,)))
    rows = mixed_own.shape[0]
    mixed_own[...] = mixture[:rows]
    mixed_other[...] = mixture[rows:].astype(jnp.bfloat16)


def vmem_call(kernel, out_shape, scalars=0, count=0):
    specs = [pl.BlockSpec(memory_space=pltpu.SMEM)] * scalars
    specs = specs + [pl.BlockSpec(memory_space=pltpu.VMEM)] * (count - scalars)
    return pl.pallas_call(
        kernel,
        out_shape=out_shape,
        in_specs=specs,
        out_specs=jax.tree.map(lambda _: pl.BlockSpec(memory_space=pltpu.VMEM), out_shape),
        compiler_params=pltpu.CompilerParams(vmem_limit_bytes=VMEM_BYTES),
    )


def shards(tokens, routes, norm_gain, router_weight, gate_up_weight, down_weight):
    rows, width = tokens.shape
    top = routes.shape[1]
    experts = router_weight.shape[1]
    devices = lax.axis_size("ep")
    shard_count = devices // experts
    if shard_count != SHARDS or experts % CORES:
        raise ValueError("unsupported mesh")
    ff = down_weight.shape[1]
    cap = min(rows, shard_count * (17 * rows * top // (16 * experts * shard_count) + 1))
    chunks = experts // CORES
    pair = CORES * cap

    index = lax.axis_index("ep")
    core = index % CORES
    expert_high = index // (CORES * shard_count)
    ids = jnp.stack(
        [(expert_high ^ m) * CORES + core for m in range(chunks)] + [core]
    ).astype(jnp.int32)

    def split(i):
        e, s = divmod(i, shard_count)
        return e // CORES, e % CORES, s // CORES, s % CORES

    def join(high, e_low, x, c):
        return ((high * CORES + e_low) * 2 + x) * CORES + c

    far = []
    for m in range(chunks):
        pairs = []
        for i in range(devices):
            high, e_low, x, c = split(i)
            pairs.append((i, join(high ^ m, c, x, e_low)))
        far.append(pairs)
    to_core = [(i, i ^ 1) for i in range(devices)]
    to_x = [(i, i ^ CORES) for i in range(devices)]

    def move(value, perm):
        return lax.ppermute(value, "ep", perm)

    other = move(tokens, to_core)
    routes = routes.T
    routes_other = move(routes, to_core)
    block = jax.ShapeDtypeStruct((pair, width), jnp.bfloat16)
    gain = norm_gain.reshape(1, width)
    normed, *blocks = vmem_call(
        functools.partial(select_kernel, experts=experts, cap=cap),
        [jax.ShapeDtypeStruct((CORES * rows, width), jnp.bfloat16)] + [block] * chunks,
        1,
        6,
    )(ids, tokens, other, routes, routes_other, gain)

    near = [move(blocks[m], far[m]) for m in range(chunks)]
    weights = jax.ShapeDtypeStruct((chunks * pair, CORES * rows), jnp.bfloat16)
    high, low = vmem_call(
        functools.partial(weight_kernel, experts=experts, cap=cap), [weights, weights], 1, 5
    )(ids, normed, router_weight.T, routes, routes_other)

    stored = gate_up_weight[0].T
    gate_up = vmem_call(
        turn_kernel, jax.ShapeDtypeStruct(stored.shape[::-1], stored.dtype), 0, 1
    )(stored)
    down = down_weight[0]
    wide = jnp.float32

    def expert(mine, other):
        mine, send = vmem_call(
            functools.partial(expert_kernel, ff=ff), [block, block], 0, 4
        )(mine, other, gate_up, down)
        return mine.astype(wide) + move(send, to_core).astype(wide)

    back = []
    for m in range(chunks):
        side = move(near[m], to_x)
        own_sum = expert(near[m], move(near[m], to_core))
        side_sum = expert(side, move(side, to_core))
        in_side = move(side_sum.astype(jnp.bfloat16), to_x)
        back.append(move((own_sum + in_side.astype(wide)).astype(jnp.bfloat16), far[m]))

    mixed_own, mixed_other = vmem_call(
        combine_kernel,
        [
            jax.ShapeDtypeStruct((rows, width), jnp.float32),
            jax.ShapeDtypeStruct((rows, width), jnp.bfloat16),
        ],
        0,
        2 + chunks,
    )(high, low, *back)
    from_other = move(mixed_other, to_core)
    return (tokens.astype(jnp.float32) + mixed_own + from_other.astype(jnp.float32)).astype(
        jnp.bfloat16
    )


def solution(mesh):
    in_specs = (
        P(("groups", "ep"), None),
        P(("groups", "ep"), None),
        P(),
        P(),
        P("ep", None, None),
        P("ep", None, None),
    )
    out_specs = P(("groups", "ep"), None)
    return jax.shard_map(shards, mesh=mesh, in_specs=in_specs, out_specs=out_specs, check_vma=False)
```

```python
import functools

import jax
import jax.numpy as jnp
from jax import lax
from jax.experimental import pallas as pl
from jax.experimental.pallas import tpu as pltpu
from jax.sharding import PartitionSpec as P


CORES = 2
SHARDS = 4
VMEM_BYTES = 16 * 1024 * 1024


def turn(m):
    return m % CORES


def dot32(a, b, dims=((1,), (0,))):
    return lax.dot_general(a, b, (dims, ((), ())), preferred_element_type=jnp.float32)


def places_of(routes_own, routes_other, own_core, experts, cap):
    places, named = [], []
    for routes, core in ((routes_own, own_core), (routes_other, 1 - own_core)):
        rows = routes.shape[1]
        ids = lax.broadcasted_iota(jnp.int32, (experts, rows), 0)
        hits = (routes[0:1, :] == ids).astype(jnp.float32)
        for k in range(1, routes.shape[0]):
            hits = hits + (routes[k : k + 1, :] == ids).astype(jnp.float32)
        before = (
            lax.broadcasted_iota(jnp.int32, (rows, rows), 0)
            < lax.broadcasted_iota(jnp.int32, (rows, rows), 1)
        ).astype(jnp.bfloat16)
        slot = dot32(hits.astype(jnp.bfloat16), before).astype(jnp.int32)
        places.append(slot + core * cap)
        named.append(hits)
    return jnp.concatenate(places, axis=1), jnp.concatenate(named, axis=1) > 0.5


def at_rows(value, expert):
    mine = lax.broadcasted_iota(jnp.int32, value.shape, 0) == expert
    return jnp.sum(jnp.where(mine, value, jnp.zeros_like(value)), axis=0, keepdims=True)


def normed_of(tokens, gain):
    stream = tokens.astype(jnp.float32)
    mean_square = jnp.mean(stream * stream, axis=-1, keepdims=True)
    return (stream * lax.rsqrt(mean_square + 1e-05) * gain).astype(jnp.bfloat16)


def select_kernel(ids, own, other, routes_own, routes_other, gain, normed, *blocks, experts, cap):
    rows = own.shape[0]
    scale = gain[...].astype(jnp.float32)
    own_core = ids[len(blocks)]
    normed[0:rows, :] = normed_of(own[...], scale)
    normed[rows:, :] = normed_of(other[...], scale)
    place, named = places_of(routes_own[...], routes_other[...], own_core, experts, cap)
    place = jnp.where(named, place + 1, 0)
    values = normed[...]
    slots = lax.broadcasted_iota(jnp.int32, (CORES * cap, CORES * rows), 0) + 1
    for m, block in enumerate(blocks):
        pick = (slots == at_rows(place, ids[m])).astype(jnp.bfloat16)
        block[...] = dot32(pick, values).astype(jnp.bfloat16)


def weight_kernel(ids, normed, router, routes_own, routes_other, high, low, *, experts, cap):
    pair = CORES * cap
    count = high.shape[0] // pair
    logits = dot32(router[...], normed[...], ((1,), (1,)))
    place, named = places_of(routes_own[...], routes_other[...], ids[count], experts, cap)
    expo = jnp.where(named, jnp.exp(logits), 0.0)
    prob = expo / jnp.sum(expo, axis=0, keepdims=True)
    place = jnp.where(named, place + 1, 0)
    slots = lax.broadcasted_iota(jnp.int32, (pair, high.shape[1]), 0) + 1
    for m in range(count):
        here = slots == at_rows(place, ids[m])
        weight = jnp.where(here, at_rows(prob, ids[m]), 0.0)
        first = weight.astype(jnp.bfloat16)
        high[m * pair : (m + 1) * pair, :] = first
        low[m * pair : (m + 1) * pair, :] = (weight - first.astype(jnp.float32)).astype(
            jnp.bfloat16
        )


def turn_kernel(stored, turned):
    turned[...] = stored[...].T


def expert_kernel(mine_in, other_in, gate_up, down, mine, send, *, ff):
    rows = mine.shape[0]
    values = jnp.concatenate([mine_in[...], other_in[...]], axis=0)
    hidden = dot32(values, gate_up[...])
    gate = hidden[:, :ff]
    up = hidden[:, ff:]
    activated = ((up + 1.0) * gate * jax.nn.sigmoid(1.702 * gate)).astype(jnp.bfloat16)
    partial_value = dot32(activated, down[...]).astype(jnp.bfloat16)
    mine[...] = partial_value[:rows]
    send[...] = partial_value[rows:]


def combine_kernel(high, low, *refs):
    mixed_own, mixed_other = refs[-2], refs[-1]
    values = jnp.concatenate([r[...] for r in refs[:-2]], axis=0)
    mixture = dot32(high[...], values, ((0,), (0,))) + dot32(low[...], values, ((0,), (0,)))
    rows = mixed_own.shape[0]
    mixed_own[...] = mixture[:rows]
    mixed_other[...] = mixture[rows:].astype(jnp.bfloat16)


def vmem_call(kernel, out_shape, scalars=0, count=0):
    specs = [pl.BlockSpec(memory_space=pltpu.SMEM)] * scalars
    specs = specs + [pl.BlockSpec(memory_space=pltpu.VMEM)] * (count - scalars)
    return pl.pallas_call(
        kernel,
        out_shape=out_shape,
        in_specs=specs,
        out_specs=jax.tree.map(lambda _: pl.BlockSpec(memory_space=pltpu.VMEM), out_shape),
        compiler_params=pltpu.CompilerParams(vmem_limit_bytes=VMEM_BYTES),
    )


def shards(tokens, routes, norm_gain, router_weight, gate_up_weight, down_weight):
    rows, width = tokens.shape
    top = routes.shape[1]
    experts = router_weight.shape[1]
    devices = lax.axis_size("ep")
    shard_count = devices // experts
    if shard_count != SHARDS or experts % CORES:
        raise ValueError("unsupported mesh")
    ff = down_weight.shape[1]
    cap = min(rows, shard_count * (17 * rows * top // (16 * experts * shard_count) + 1))
    chunks = experts // CORES
    pair = CORES * cap

    index = lax.axis_index("ep")
    core = index % CORES
    expert_high = index // (CORES * shard_count)
    ids = jnp.stack(
        [(expert_high ^ m) * CORES + (core ^ turn(m)) for m in range(chunks)] + [core]
    ).astype(jnp.int32)

    def split(i):
        e, s = divmod(i, shard_count)
        return e // CORES, e % CORES, s // CORES, s % CORES

    def join(high, e_low, x, c):
        return ((high * CORES + e_low) * 2 + x) * CORES + c

    far = []
    for m in range(chunks):
        pairs = []
        for i in range(devices):
            high, e_low, x, c = split(i)
            pairs.append((i, join(high ^ m, c ^ turn(m), x, e_low ^ turn(m))))
        far.append(pairs)
    to_core = [(i, i ^ 1) for i in range(devices)]
    to_x = [(i, i ^ CORES) for i in range(devices)]

    def move(value, perm):
        return lax.ppermute(value, "ep", perm)

    other = move(tokens, to_core)
    routes = routes.T
    routes_other = move(routes, to_core)
    block = jax.ShapeDtypeStruct((pair, width), jnp.bfloat16)
    gain = norm_gain.reshape(1, width)
    normed, *blocks = vmem_call(
        functools.partial(select_kernel, experts=experts, cap=cap),
        [jax.ShapeDtypeStruct((CORES * rows, width), jnp.bfloat16)] + [block] * chunks,
        1,
        6,
    )(ids, tokens, other, routes, routes_other, gain)

    near = [move(blocks[m], far[m]) for m in range(chunks)]
    weights = jax.ShapeDtypeStruct((chunks * pair, CORES * rows), jnp.bfloat16)
    high, low = vmem_call(
        functools.partial(weight_kernel, experts=experts, cap=cap), [weights, weights], 1, 5
    )(ids, normed, router_weight.T, routes, routes_other)

    stored = gate_up_weight[0].T
    gate_up = vmem_call(
        turn_kernel, jax.ShapeDtypeStruct(stored.shape[::-1], stored.dtype), 0, 1
    )(stored)
    down = down_weight[0]
    wide = jnp.float32

    def expert(mine, other):
        mine, send = vmem_call(
            functools.partial(expert_kernel, ff=ff), [block, block], 0, 4
        )(mine, other, gate_up, down)
        return mine.astype(wide) + move(send, to_core).astype(wide)

    back = []
    for m in range(chunks):
        side = move(near[m], to_x)
        own_sum = expert(near[m], move(near[m], to_core))
        side_sum = expert(side, move(side, to_core))
        in_side = move(side_sum.astype(jnp.bfloat16), to_x)
        back.append(move((own_sum + in_side.astype(wide)).astype(jnp.bfloat16), far[m]))

    mixed_own, mixed_other = vmem_call(
        combine_kernel,
        [
            jax.ShapeDtypeStruct((rows, width), jnp.float32),
            jax.ShapeDtypeStruct((rows, width), jnp.bfloat16),
        ],
        0,
        2 + chunks,
    )(high, low, *back)
    from_other = move(mixed_other, to_core)
    return (tokens.astype(jnp.float32) + mixed_own + from_other.astype(jnp.float32)).astype(
        jnp.bfloat16
    )


def solution(mesh):
    in_specs = (
        P(("groups", "ep"), None),
        P(("groups", "ep"), None),
        P(),
        P(),
        P("ep", None, None),
        P("ep", None, None),
    )
    out_specs = P(("groups", "ep"), None)
    return jax.shard_map(shards, mesh=mesh, in_specs=in_specs, out_specs=out_specs, check_vma=False)
```
